32 devices in a mesh: scene: 2 (over x), view: 16 (over z, y, core).
Axes of the slice: x: 2, y: 2, z: 4, core: 2. Of those that a mesh axis runs over, the one named last changes fastest.
Arguments:
- latents: bfloat16 [256, 64, 512], P(('scene', 'view')), parts along dimension 0, may hold values from -48 to 48
- norm_gain: float32 [512], replicated, may hold values from 0.1 to 1.9
- norm_shift: float32 [512], replicated, may hold values from -3 to 3
- w_first: bfloat16 [512, 3, 3, 512], replicated, may hold values from -0.09375 to 0.09375
- bias_first: float32 [512], replicated, may hold values from -3 to 3
- w_second: bfloat16 [512, 3, 3, 512], replicated, may hold values from -0.09375 to 0.09375
- bias_second: float32 [512], replicated, may hold values from -3 to 3
Outputs:
- decoded: bfloat16 [512, 128, 512], P(('scene', 'view')), parts along dimension 0
The draws below stay inside these ranges and needn't reach their ends.
There are 2 independent parts, one for each index of `scene`. The reference program is written for one: setup_inputs(seed, part) draws one part's arguments, and reference() takes and returns one part's arrays. A program takes and returns all parts, laid end to end along the dimension named above; an argument that names none is the same for every part. Nothing has to cross between parts.
All inputs are finite; a program needn't handle non-finite values.
Results may differ from the reference program's by a relative error of at most 0.0051.
Values may be sent and summed in bfloat16 or wider, within the bound.
A program may use at most 128 MiB of HBM per device.

```python
import jax
import jax.numpy as jnp
from jax import lax

C = 512
GROUPS = 32
ROWS_DEV = 8
H_LAT = 32
W_LAT = 64
SLABS = 4
VIEWS = 4


def draw_latents(key, part):
    total_rows = VIEWS * H_LAT
    block_count = total_rows // ROWS_DEV
    key_noise = jax.random.fold_in(key, 11)
    key_scale = jax.random.fold_in(key, 23)
    key_level = jax.random.fold_in(key, 37)
    key_sign = jax.random.fold_in(key, 41)
    key_jitter = jax.random.fold_in(key, 53)
    key_block_sign = jax.random.fold_in(key, 61)
    key_block_level = jax.random.fold_in(key, 67)
    key_block_noise = jax.random.fold_in(key, 71)
    noise = jnp.clip(jax.random.normal(key_noise, (total_rows, W_LAT, C), jnp.float32), -4.0, 4.0)
    place = jnp.arange(total_rows, dtype=jnp.float32) / (total_rows - 1)
    level = jax.random.uniform(key_level, (GROUPS,), jnp.float32, 0.5, 1.5)
    sign = jnp.where(jax.random.uniform(key_sign, (GROUPS,), jnp.float32) < 0.5, -1.0, 1.0)
    block_sign = jnp.where(jax.random.uniform(key_block_sign, (block_count, GROUPS), jnp.float32) < 0.5, -1.0, 1.0)
    chan_jitter = jax.random.uniform(key_jitter, (C,), jnp.float32, 0.7, 1.3)
    row_scale = 3.0 ** (place - 0.5)
    chan_scale = 2.0 ** (2.0 * jax.random.uniform(key_scale, (C,), jnp.float32) - 1.0)
    rise = 1.0 + 2.0 * place
    block_level = jax.random.uniform(key_block_level, (block_count, GROUPS), jnp.float32, 0.3, 1.7)
    block_noise = jax.random.uniform(key_block_noise, (block_count,), jnp.float32, 0.5, 1.5)
    common = 0.5
    block_group = common * (level * sign)[None, :] + block_sign * block_level
    block_shift = jnp.broadcast_to(block_group[:, :, None], (block_count, GROUPS, C // GROUPS)).reshape(block_count, C) * chan_jitter
    row_shift = jnp.repeat(block_shift, ROWS_DEV, axis=0)
    row_noise = jnp.repeat(block_noise, ROWS_DEV, axis=0)
    values = noise * (row_scale * row_noise)[:, None, None] * chan_scale + rise[:, None, None] * row_shift[:, None, :]
    values = jnp.clip(0.35 * values, -48.0, 48.0)
    return values.astype(jnp.bfloat16)


def normal_values(key, shape, spread, most, kind=jnp.bfloat16):
    entries = spread * jax.random.normal(key, shape, jnp.float32)
    return jnp.clip(entries, min=-most, max=most).astype(kind)


def setup_inputs(seed: int = 0, part: int = 0) -> dict:
    key_of = jax.random.split(jax.random.key(seed), 8)
    part_keys = jax.random.split(jax.random.fold_in(key_of[7], part), 8)
    latents = draw_latents(jax.random.fold_in(jax.random.fold_in(key_of[7], part), 71), part)
    norm_gain = jnp.clip(1.0 + 0.18 * jax.random.normal(key_of[1], (C,), jnp.float32), 0.1, 1.9)
    norm_shift = normal_values(key_of[2], (C,), 0.5, 3.0, jnp.float32)
    w_first = normal_values(key_of[3], (C, 3, 3, C), (9 * C) ** -0.5, 0.09375)
    bias_first = normal_values(key_of[4], (C,), 0.5, 3.0, jnp.float32)
    w_second = normal_values(key_of[5], (C, 3, 3, C), (9 * C) ** -0.5, 0.09375)
    bias_second = normal_values(key_of[6], (C,), 0.5, 3.0, jnp.float32)
    return dict(latents=latents, norm_gain=norm_gain, norm_shift=norm_shift, w_first=w_first, bias_first=bias_first, w_second=w_second, bias_second=bias_second)


epsilon = 1e-06

def convolve(inputs, filters):
    return lax.conv_general_dilated(inputs.astype(jnp.float32), filters.astype(jnp.float32), (1, 1), ((1, 1), (1, 1)), dimension_numbers=('NHWC', 'OHWI', 'NHWC'), precision=lax.Precision.HIGHEST)

def reference(latents, norm_gain, norm_shift, w_first, bias_first, w_second, bias_second):
    per_group = C // GROUPS
    values = latents.astype(jnp.float32).reshape(SLABS, VIEWS, ROWS_DEV, W_LAT, C)
    values = jnp.transpose(values, (1, 0, 2, 3, 4)).reshape(VIEWS, H_LAT, W_LAT, C)
    grouped = values.reshape(VIEWS, H_LAT, W_LAT, GROUPS, per_group)
    group_mean = lax.optimization_barrier(jnp.mean(grouped, axis=(0, 1, 2, 4), keepdims=True))
    group_var = lax.optimization_barrier(jnp.mean(jnp.square(grouped - group_mean), axis=(0, 1, 2, 4), keepdims=True))
    normed = ((grouped - group_mean) * lax.rsqrt(group_var + epsilon)).reshape(VIEWS, H_LAT, W_LAT, C)
    active = jax.nn.silu(normed * norm_gain + norm_shift).astype(jnp.bfloat16)
    mixed = (values + convolve(active, w_first) + bias_first).astype(jnp.bfloat16)
    doubled = jnp.repeat(jnp.repeat(mixed, 2, axis=1), 2, axis=2)
    decoded = (convolve(doubled, w_second) + bias_second).astype(jnp.bfloat16)
    decoded = decoded.reshape(VIEWS, SLABS, 2 * ROWS_DEV, 2 * W_LAT, C)
    decoded = jnp.transpose(decoded, (1, 0, 2, 3, 4))
    return decoded.reshape(VIEWS * 2 * H_LAT, 2 * W_LAT, C)
```

```python
import functools

import jax
import jax.numpy as jnp
from jax import lax
from jax.experimental import pallas as pl
from jax.experimental.pallas import tpu as pltpu
from jax.sharding import PartitionSpec as P

GROUPS = 32
H_LAT = 32
EPSILON = 1e-06
LANES = 128
F32 = jnp.float32
BF16 = jnp.bfloat16


def dot_nt(x, w):
    return lax.dot_general(x, w, (((1,), (1,)), ((), ())), preferred_element_type=F32)


def kernel(
    n_view, rows, cols, chans,
    lat_hbm, gain_ref, shift_ref, w1_hbm, b1_ref, w2_hbm, b2_ref,
    out_ref,
    lat, w1, w2, fold, act, acc, lhs_m, lhs_u, part, wide, stat, stat_in,
    lat_sem, w1_sem, w2_sem, halo_send, halo_recv, stat_send, stat_recv,
):
    me = lax.axis_index("view")
    slabs = H_LAT // rows
    views = n_view // slabs
    slab = me // views
    own = rows * cols
    ext = (rows + 2) * cols
    has_up = slab > 0
    has_down = slab < slabs - 1

    own_copy = pltpu.make_async_copy(lat_hbm, lat.at[pl.ds(2, rows)], lat_sem)
    own_copy.start()

    barrier = pltpu.get_barrier_semaphore()

    def greet(k, carry):
        pl.semaphore_signal(barrier, inc=1, device_id={"view": lax.rem(me + k, n_view)})
        return carry

    lax.fori_loop(1, n_view, greet, 0)

    def w1_copy(t):
        return pltpu.make_async_copy(w1_hbm.at[t], w1.at[t], w1_sem.at[t])

    def w2_copy(t):
        return pltpu.make_async_copy(w2_hbm.at[t], w2.at[t], w2_sem.at[t])

    for t in range(9):
        w1_copy(t).start()
    for t in range(9):
        w2_copy(t).start()

    own_copy.wait()

    def add_row(i, carry):
        x = lat[2 + i].astype(F32).reshape(cols // 8, 8, chans)
        return carry[0] + jnp.sum(x, axis=0), carry[1] + jnp.sum(x * x, axis=0)

    zero = jnp.zeros((8, chans), F32)
    sums, squares = lax.fori_loop(0, rows, add_row, (zero, zero))
    sums = jnp.sum(sums, axis=0, keepdims=True)
    squares = jnp.sum(squares, axis=0, keepdims=True)
    blocks = chans // LANES
    packed = jnp.concatenate(
        [v[:, k * LANES : (k + 1) * LANES] for v in (sums, squares) for k in range(blocks)], axis=0
    )
    lane = lax.broadcasted_iota(jnp.int32, packed.shape, 1)
    step = 1
    while step < chans // GROUPS:
        packed = packed + jnp.where(
            (lane & step) == 0,
            pltpu.roll(packed, LANES - step, 1),
            pltpu.roll(packed, step, 1),
        )
        step *= 2
    stat[...] = packed

    pl.semaphore_wait(barrier, n_view - 1)

    def stat_copy(k):
        return pltpu.make_async_remote_copy(
            src_ref=stat, dst_ref=stat_in.at[k - 1], send_sem=stat_send, recv_sem=stat_recv,
            device_id={"view": lax.rem(me + k, n_view)},
        )

    def send_stat(k, carry):
        stat_copy(k).start()
        return carry

    lax.fori_loop(1, n_view, send_stat, 0)

    up_copy = pltpu.make_async_remote_copy(
        src_ref=lat_hbm.at[pl.ds(0, 2)], dst_ref=lat.at[pl.ds(rows + 2, 2)],
        send_sem=halo_send.at[0], recv_sem=halo_recv.at[0],
        device_id={"view": jnp.maximum(me - views, 0)},
    )
    down_copy = pltpu.make_async_remote_copy(
        src_ref=lat_hbm.at[pl.ds(rows - 2, 2)], dst_ref=lat.at[pl.ds(0, 2)],
        send_sem=halo_send.at[1], recv_sem=halo_recv.at[1],
        device_id={"view": jnp.minimum(me + views, n_view - 1)},
    )

    @pl.when(has_up)
    def _():
        up_copy.start()

    @pl.when(has_down)
    def _():
        down_copy.start()

    pltpu.make_async_copy(stat_in, stat_in, stat_recv).wait()

    total = stat[...]
    total = total + jnp.sum(stat_in[...], axis=0)
    entries = float(own * (chans // GROUPS) * n_view)
    mean = total[:blocks] / entries
    var = total[blocks:] / entries - mean * mean
    inv = lax.rsqrt(var + EPSILON)

    def one_row(v):
        return jnp.concatenate([v[k : k + 1] for k in range(blocks)], axis=1)

    scale = one_row(inv) * gain_ref[...]
    offset = shift_ref[...] - one_row(mean) * scale

    @pl.when(has_up)
    def _():
        down_copy.wait_recv()

    @pl.when(has_down)
    def _():
        up_copy.wait_recv()

    col = lax.broadcasted_iota(jnp.int32, (cols, chans), 0)

    def left_of(x):
        return jnp.where(col == 0, 0.0, pltpu.roll(x, 1, 0))

    def right_of(x):
        return jnp.where(col == cols - 1, 0.0, pltpu.roll(x, cols - 1, 0))

    half_scale = scale * 0.5
    half_offset = offset * 0.5

    def activate(i, carry):
        h = lat[i].astype(F32) * half_scale + half_offset
        a = h + h * jnp.tanh(h)
        place = slab * rows + i - 2
        a = jnp.where(jnp.logical_and(place >= 0, place < H_LAT), a, 0.0)
        at = pl.ds(pl.multiple_of(i * cols, cols), cols)
        act[0, at] = left_of(a).astype(BF16)
        act[1, at] = a.astype(BF16)
        act[2, at] = right_of(a).astype(BF16)
        return carry

    lax.fori_loop(0, rows + 4, activate, 0)

    def tap(t, carry):
        w1_copy(t).wait()
        r = t // 3
        s = t - 3 * r
        x = act[s, pl.ds(pl.multiple_of(r * cols, cols), ext)]
        term = dot_nt(x, w1[t])

        @pl.when(t == 0)
        def _():
            acc[...] = term

        @pl.when(t > 0)
        def _():
            acc[...] += term

        return carry

    lax.fori_loop(0, 9, tap, 0)

    for t in range(9):
        w2_copy(t).wait()
    piece = 32

    def fold_piece(k, carry):
        at = pl.ds(pl.multiple_of(k * piece, piece), piece)
        w = [w2[t, at].astype(F32) for t in range(9)]
        by_col = [w[s] + w[3 + s] + w[6 + s] for s in range(3)]
        fold[0, at] = (by_col[0] + by_col[1] + by_col[2]).astype(BF16)
        fold[1, at] = by_col[0].astype(BF16)
        fold[2, at] = by_col[2].astype(BF16)
        fold[3, at] = (w[0] + w[1] + w[2]).astype(BF16)
        fold[4, at] = (w[6] + w[7] + w[8]).astype(BF16)
        return carry

    lax.fori_loop(0, chans // piece, fold_piece, 0)

    bias1 = b1_ref[...]

    def mixed_row(i):
        at = pl.ds(pl.multiple_of(i * cols, cols), cols)
        m = lat[i + 1].astype(F32) + acc[at] + bias1
        m = m.astype(BF16).astype(F32)
        place = slab * rows + i - 1
        return jnp.where(jnp.logical_and(place >= 0, place < H_LAT), m, 0.0)

    def spread(i, carry):
        m = mixed_row(i + 1)
        u = m - mixed_row(i)
        at = pl.ds(pl.multiple_of(i * cols, cols), cols)
        for ref, x in ((lhs_m, m), (lhs_u, u)):
            ref[0, at] = x.astype(BF16)
            ref[1, at] = (left_of(x) - x).astype(BF16)
            ref[2, at] = (right_of(x) - x).astype(BF16)
        return carry

    lax.fori_loop(0, rows + 1, spread, 0)

    width = 256

    def out_tile(n, carry):
        lanes = pl.ds(pl.multiple_of(n * width, width), width)
        head = pl.ds(0, own)
        base = dot_nt(lhs_m[0, head], fold[0, lanes]) + b2_ref[:, lanes]
        part[0] = base + dot_nt(lhs_m[1, head], fold[1, lanes])
        part[1] = base + dot_nt(lhs_m[2, head], fold[2, lanes])
        for p in range(2):
            at = pl.ds(p * cols, own)
            rise = dot_nt(lhs_u[0, at], fold[3 + p, lanes])
            for q in range(2):
                term = rise + dot_nt(lhs_u[1 + q, at], w2[6 * p + 2 * q, lanes])
                value = part[q] + term if p else part[q] - term
                for g in range(width // LANES):
                    wide[g, pl.ds(p * own * 2 + q, own, 2), :] = value[:, g * LANES : (g + 1) * LANES]
        for p in range(2):
            for g in range(width // LANES):
                tile = wide[g, pl.ds(p * own * 2, own * 2), :].astype(BF16)
                out_ref[:, p, :, pl.ds(pl.multiple_of(n * width + g * LANES, LANES), LANES)] = tile.reshape(
                    rows, 2 * cols, LANES
                )
        return carry

    lax.fori_loop(0, chans // width, out_tile, 0)

    pltpu.make_async_copy(stat_in, stat_in, stat_send).wait()

    @pl.when(has_up)
    def _():
        up_copy.wait_send()

    @pl.when(has_down)
    def _():
        down_copy.wait_send()


def per_device(n_view, latents, norm_gain, norm_shift, w_first, bias_first, w_second, bias_second):
    rows, cols, chans = latents.shape
    own = rows * cols
    flat = lambda w: jnp.transpose(w, (1, 2, 0, 3)).reshape(9, chans, chans)
    row = lambda v: v.reshape(1, chans)
    vmem = pl.BlockSpec(memory_space=pltpu.VMEM)
    hbm = pl.BlockSpec(memory_space=pl.ANY)
    out = pl.pallas_call(
        functools.partial(kernel, n_view, rows, cols, chans),
        out_shape=jax.ShapeDtypeStruct((rows, 2, 2 * cols, chans), BF16),
        in_specs=[hbm, vmem, vmem, hbm, vmem, hbm, vmem],
        out_specs=vmem,
        scratch_shapes=[
            pltpu.VMEM((rows + 4, cols, chans), BF16),
            pltpu.VMEM((9, chans, chans), BF16),
            pltpu.VMEM((9, chans, chans), BF16),
            pltpu.VMEM((5, chans, chans), BF16),
            pltpu.VMEM((3, (rows + 4) * cols, chans), BF16),
            pltpu.VMEM(((rows + 2) * cols, chans), F32),
            pltpu.VMEM((3, own + cols, chans), BF16),
            pltpu.VMEM((3, own + cols, chans), BF16),
            pltpu.VMEM((2, own, 256), F32),
            pltpu.VMEM((2, own * 4, LANES), F32),
            pltpu.VMEM((2 * chans // LANES, LANES), F32),
            pltpu.VMEM((n_view - 1, 2 * chans // LANES, LANES), F32),
            pltpu.SemaphoreType.DMA,
            pltpu.SemaphoreType.DMA((9,)),
            pltpu.SemaphoreType.DMA((9,)),
            pltpu.SemaphoreType.DMA((2,)),
            pltpu.SemaphoreType.DMA((2,)),
            pltpu.SemaphoreType.DMA,
            pltpu.SemaphoreType.DMA,
        ],
        compiler_params=pltpu.CompilerParams(
            collective_id=0, has_side_effects=True, vmem_limit_bytes=60 * 1024 * 1024
        ),
    )(
        latents, row(norm_gain), row(norm_shift), flat(w_first), row(bias_first), flat(w_second),
        row(bias_second),
    )
    return out.reshape(2 * rows, 2 * cols, chans)


def solution(mesh):
    placed = (P(("scene", "view"), None, None), P(), P(), P(), P(), P(), P())
    return jax.shard_map(
        functools.partial(per_device, mesh.shape["view"]),
        mesh=mesh,
        in_specs=placed,
        out_specs=P(("scene", "view"), None, None),
        check_vma=False,
    )
```

```python
import functools

import jax
import jax.numpy as jnp
from jax import lax
from jax.experimental import pallas as pl
from jax.experimental.pallas import tpu as pltpu
from jax.sharding import PartitionSpec as P

GROUPS = 32
H_LAT = 32
EPSILON = 1e-06
LANES = 128
F32 = jnp.float32
BF16 = jnp.bfloat16


def dot_nt(x, w):
    return lax.dot_general(x, w, (((1,), (1,)), ((), ())), preferred_element_type=F32)


def kernel(
    n_view, rows, cols, chans,
    lat_hbm, gain_ref, shift_ref, w1_hbm, b1_ref, w2_hbm, b2_ref,
    out_ref,
    lat, w1, w2, fold, act, acc, lhs_m, lhs_u, part, wide, stat, stat_in,
    lat_sem, w1_sem, w2_sem, halo_send, halo_recv, stat_send, stat_recv,
):
    me = lax.axis_index("view")
    slabs = H_LAT // rows
    views = n_view // slabs
    slab = me // views
    own = rows * cols
    has_up = slab > 0
    has_down = slab < slabs - 1

    own_copy = pltpu.make_async_copy(lat_hbm, lat.at[pl.ds(2, rows)], lat_sem)
    own_copy.start()

    barrier = pltpu.get_barrier_semaphore()

    def greet(k, carry):
        pl.semaphore_signal(barrier, inc=1, device_id={"view": lax.rem(me + k, n_view)})
        return carry

    lax.fori_loop(1, n_view, greet, 0, unroll=n_view <= 16)

    def w1_copy(t):
        return pltpu.make_async_copy(w1_hbm.at[t], w1.at[:, pl.ds(t * chans, chans)], w1_sem.at[t])

    def w2_copy(t):
        return pltpu.make_async_copy(w2_hbm.at[t], w2.at[t], w2_sem.at[t])

    for t in range(9):
        w1_copy(t).start()
    for t in range(9):
        w2_copy(t).start()

    own_copy.wait()

    def add_row(i, carry):
        x = lat[2 + i].astype(F32).reshape(cols // 8, 8, chans)
        return carry[0] + jnp.sum(x, axis=0), carry[1] + jnp.sum(x * x, axis=0)

    zero = jnp.zeros((8, chans), F32)
    sums, squares = lax.fori_loop(0, rows, add_row, (zero, zero))
    sums = jnp.sum(sums, axis=0, keepdims=True)
    squares = jnp.sum(squares, axis=0, keepdims=True)
    blocks = chans // LANES
    packed = jnp.concatenate(
        [v[:, k * LANES : (k + 1) * LANES] for v in (sums, squares) for k in range(blocks)], axis=0
    )
    lane = lax.broadcasted_iota(jnp.int32, packed.shape, 1)
    step = 1
    while step < chans // GROUPS:
        packed = packed + jnp.where(
            (lane & step) == 0,
            pltpu.roll(packed, LANES - step, 1),
            pltpu.roll(packed, step, 1),
        )
        step *= 2
    stat[...] = packed

    pl.semaphore_wait(barrier, n_view - 1)

    def stat_copy(k):
        return pltpu.make_async_remote_copy(
            src_ref=stat, dst_ref=stat_in.at[k - 1], send_sem=stat_send, recv_sem=stat_recv,
            device_id={"view": lax.rem(me + k, n_view)},
        )

    def send_stat(k, carry):
        stat_copy(k).start()
        return carry

    lax.fori_loop(1, n_view, send_stat, 0, unroll=n_view <= 16)

    up_copy = pltpu.make_async_remote_copy(
        src_ref=lat_hbm.at[pl.ds(0, 2)], dst_ref=lat.at[pl.ds(rows + 2, 2)],
        send_sem=halo_send.at[0], recv_sem=halo_recv.at[0],
        device_id={"view": jnp.maximum(me - views, 0)},
    )
    down_copy = pltpu.make_async_remote_copy(
        src_ref=lat_hbm.at[pl.ds(rows - 2, 2)], dst_ref=lat.at[pl.ds(0, 2)],
        send_sem=halo_send.at[1], recv_sem=halo_recv.at[1],
        device_id={"view": jnp.minimum(me + views, n_view - 1)},
    )

    @pl.when(has_up)
    def _():
        up_copy.start()

    @pl.when(has_down)
    def _():
        down_copy.start()

    for t in range(9):
        w2_copy(t).wait()
    piece = 32

    def fold_piece(k, carry):
        at = pl.ds(pl.multiple_of(k * piece, piece), piece)
        w = [w2[t, at].astype(F32) for t in range(9)]
        by_col = [w[s] + w[3 + s] + w[6 + s] for s in range(3)]
        fold[0, at] = (by_col[0] + by_col[1] + by_col[2]).astype(BF16)
        fold[1, at] = by_col[0].astype(BF16)
        fold[2, at] = by_col[2].astype(BF16)
        fold[3, at] = (w[0] + w[1] + w[2]).astype(BF16)
        fold[4, at] = (w[6] + w[7] + w[8]).astype(BF16)
        return carry

    lax.fori_loop(0, chans // piece, fold_piece, 0)

    pltpu.make_async_copy(stat_in, stat_in, stat_recv).wait()

    total = stat[...]
    total = total + jnp.sum(stat_in[...], axis=0)
    entries = float(own * (chans // GROUPS) * n_view)
    mean = total[:blocks] / entries
    var = total[blocks:] / entries - mean * mean
    inv = lax.rsqrt(var + EPSILON)

    def one_row(v):
        return jnp.concatenate([v[k : k + 1] for k in range(blocks)], axis=1)

    scale = one_row(inv) * gain_ref[...]
    offset = shift_ref[...] - one_row(mean) * scale

    col = lax.broadcasted_iota(jnp.int32, (cols, chans), 0)

    def left_of(x):
        return jnp.where(col == 0, 0.0, pltpu.roll(x, 1, 0))

    def right_of(x):
        return jnp.where(col == cols - 1, 0.0, pltpu.roll(x, cols - 1, 0))

    half_scale = scale * 0.5
    half_offset = offset * 0.5

    def activate(i, carry):
        h = lat[i].astype(F32) * half_scale + half_offset
        a = h + h * jnp.tanh(h)
        place = slab * rows + i - 2
        a = jnp.where(jnp.logical_and(place >= 0, place < H_LAT), a, 0.0)
        at = pl.ds(pl.multiple_of(i * cols, cols), cols)
        act[at, pl.ds(0, chans)] = left_of(a).astype(BF16)
        act[at, pl.ds(chans, chans)] = a.astype(BF16)
        act[at, pl.ds(2 * chans, chans)] = right_of(a).astype(BF16)
        return carry

    lax.fori_loop(2, rows + 2, activate, 0)
    for t in range(9):
        w1_copy(t).wait()
    deep = 3 * chans
    half = 256

    def taps(windows, n):
        lanes = pl.ds(n * half, half)
        terms = [
            dot_nt(
                jnp.concatenate([act[pl.ds(first + r * cols, size)] for first, size in windows], axis=0),
                w1[lanes, pl.ds(r * deep, deep)],
            )
            for r in range(3)
        ]
        return terms[0] + terms[1] + terms[2]

    for n in range(chans // half):
        acc[pl.ds(2 * cols, own - 2 * cols), pl.ds(n * half, half)] = taps([(2 * cols, own - 2 * cols)], n)

    @pl.when(has_up)
    def _():
        down_copy.wait_recv()

    @pl.when(has_down)
    def _():
        up_copy.wait_recv()

    lax.fori_loop(0, 2, activate, 0)
    lax.fori_loop(rows + 2, rows + 4, activate, 0)
    ends = [(0, 2 * cols), (own, 2 * cols)]
    for n in range(chans // half):
        term = taps(ends, n)
        for k, (first, size) in enumerate(ends):
            acc[pl.ds(first, size), pl.ds(n * half, half)] = term[k * size : (k + 1) * size]

    bias1 = b1_ref[...]

    def mixed_row(i):
        at = pl.ds(pl.multiple_of(i * cols, cols), cols)
        m = lat[i + 1].astype(F32) + acc[at] + bias1
        m = m.astype(BF16).astype(F32)
        place = slab * rows + i - 1
        return jnp.where(jnp.logical_and(place >= 0, place < H_LAT), m, 0.0)

    def spread(i, carry):
        m = mixed_row(i + 1)
        u = m - mixed_row(i)
        at = pl.ds(pl.multiple_of(i * cols, cols), cols)
        for ref, x in ((lhs_m, m), (lhs_u, u)):
            ref[0, at] = x.astype(BF16)
            ref[1, at] = (left_of(x) - x).astype(BF16)
            ref[2, at] = (right_of(x) - x).astype(BF16)
        return carry

    lax.fori_loop(0, rows + 1, spread, 0)

    width = 256

    for n in range(chans // width):
        lanes = pl.ds(n * width, width)
        head = pl.ds(0, own)
        base = dot_nt(lhs_m[0, head], fold[0, lanes]) + b2_ref[:, lanes]
        part[0] = base + dot_nt(lhs_m[1, head], fold[1, lanes])
        part[1] = base + dot_nt(lhs_m[2, head], fold[2, lanes])
        for p in range(2):
            at = pl.ds(p * cols, own)
            rise = dot_nt(lhs_u[0, at], fold[3 + p, lanes])
            for q in range(2):
                term = rise + dot_nt(lhs_u[1 + q, at], w2[6 * p + 2 * q, lanes])
                value = part[q] + term if p else part[q] - term
                for g in range(width // LANES):
                    wide[g, pl.ds(p * own * 2 + q, own, 2), :] = value[:, g * LANES : (g + 1) * LANES]
            for g in range(width // LANES):
                tile = wide[g, pl.ds(p * own * 2, own * 2), :].astype(BF16)
                out_ref[:, p, :, pl.ds(n * width + g * LANES, LANES)] = tile.reshape(rows, 2 * cols, LANES)

    pltpu.make_async_copy(stat_in, stat_in, stat_send).wait()

    @pl.when(has_up)
    def _():
        up_copy.wait_send()

    @pl.when(has_down)
    def _():
        down_copy.wait_send()


def per_device(n_view, latents, norm_gain, norm_shift, w_first, bias_first, w_second, bias_second):
    rows, cols, chans = latents.shape
    own = rows * cols
    flat = lambda w: jnp.transpose(w, (1, 2, 0, 3)).reshape(9, chans, chans)
    row = lambda v: v.reshape(1, chans)
    vmem = pl.BlockSpec(memory_space=pltpu.VMEM)
    hbm = pl.BlockSpec(memory_space=pl.ANY)
    out = pl.pallas_call(
        functools.partial(kernel, n_view, rows, cols, chans),
        out_shape=pltpu.VMEM((rows, 2, 2 * cols, chans), BF16),
        in_specs=[hbm, vmem, vmem, hbm, vmem, hbm, vmem],
        out_specs=vmem,
        scratch_shapes=[
            pltpu.VMEM((rows + 4, cols, chans), BF16),
            pltpu.VMEM((chans, 9 * chans), BF16),
            pltpu.VMEM((9, chans, chans), BF16),
            pltpu.VMEM((5, chans, chans), BF16),
            pltpu.VMEM(((rows + 4) * cols, 3 * chans), BF16),
            pltpu.VMEM(((rows + 2) * cols, chans), F32),
            pltpu.VMEM((3, own + cols, chans), BF16),
            pltpu.VMEM((3, own + cols, chans), BF16),
            pltpu.VMEM((2, own, 256), F32),
            pltpu.VMEM((2, own * 4, LANES), F32),
            pltpu.VMEM((2 * chans // LANES, LANES), F32),
            pltpu.VMEM((n_view - 1, 2 * chans // LANES, LANES), F32),
            pltpu.SemaphoreType.DMA,
            pltpu.SemaphoreType.DMA((9,)),
            pltpu.SemaphoreType.DMA((9,)),
            pltpu.SemaphoreType.DMA((2,)),
            pltpu.SemaphoreType.DMA((2,)),
            pltpu.SemaphoreType.DMA,
            pltpu.SemaphoreType.DMA,
        ],
        compiler_params=pltpu.CompilerParams(
            collective_id=0, has_side_effects=True, vmem_limit_bytes=60 * 1024 * 1024
        ),
    )(
        latents, row(norm_gain), row(norm_shift), flat(w_first), row(bias_first), flat(w_second),
        row(bias_second),
    )
    return out.reshape(2 * rows, 2 * cols, chans)


def solution(mesh):
    placed = (P(("scene", "view"), None, None), P(), P(), P(), P(), P(), P())
    return jax.shard_map(
        functools.partial(per_device, mesh.shape["view"]),
        mesh=mesh,
        in_specs=placed,
        out_specs=P(("scene", "view"), None, None),
        check_vma=False,
    )
```

```python
import functools

import jax
import jax.numpy as jnp
from jax import lax
from jax.experimental import pallas as pl
from jax.experimental.pallas import tpu as pltpu
from jax.sharding import PartitionSpec as P

GROUPS = 32
H_LAT = 32
EPSILON = 1e-06
LANES = 128
F32 = jnp.float32
BF16 = jnp.bfloat16


def dot_nt(x, w):
    return lax.dot_general(x, w, (((1,), (1,)), ((), ())), preferred_element_type=F32)


def kernel(
    n_view, rows, cols, chans,
    lat_hbm, gain_ref, shift_ref, w1_hbm, b1_ref, w2_hbm, b2_ref,
    out_ref,
    lat, w1, w2, fold, act, acc, lhs_m, lhs_u, part, wide, stat, stat_in,
    lat_sem, w1_sem, w2_sem, halo_send, halo_recv, stat_send, stat_recv,
):
    me = lax.axis_index("view")
    slabs = H_LAT // rows
    views = n_view // slabs
    slab = me // views
    own = rows * cols
    has_up = slab > 0
    has_down = slab < slabs - 1

    own_copy = pltpu.make_async_copy(lat_hbm, lat.at[pl.ds(2, rows)], lat_sem)
    own_copy.start()

    barrier = pltpu.get_barrier_semaphore()

    def greet(k, carry):
        pl.semaphore_signal(barrier, inc=1, device_id={"view": lax.rem(me + k, n_view)})
        return carry

    lax.fori_loop(1, n_view, greet, 0, unroll=n_view <= 16)

    def w1_copy(t):
        return pltpu.make_async_copy(w1_hbm.at[t], w1.at[:, pl.ds(t * chans, chans)], w1_sem.at[t])

    def w2_copy(t):
        return pltpu.make_async_copy(w2_hbm.at[t], w2.at[t], w2_sem.at[t])

    for t in range(9):
        w1_copy(t).start()
    for t in range(9):
        w2_copy(t).start()

    own_copy.wait()

    def add_row(i, carry):
        x = lat[2 + i].astype(F32).reshape(cols // 8, 8, chans)
        return carry[0] + jnp.sum(x, axis=0), carry[1] + jnp.sum(x * x, axis=0)

    zero = jnp.zeros((8, chans), F32)
    sums, squares = lax.fori_loop(0, rows, add_row, (zero, zero))
    sums = jnp.sum(sums, axis=0, keepdims=True)
    squares = jnp.sum(squares, axis=0, keepdims=True)
    blocks = chans // LANES
    packed = jnp.concatenate(
        [v[:, k * LANES : (k + 1) * LANES] for v in (sums, squares) for k in range(blocks)], axis=0
    )
    lane = lax.broadcasted_iota(jnp.int32, packed.shape, 1)
    step = 1
    while step < chans // GROUPS:
        packed = packed + jnp.where(
            (lane & step) == 0,
            pltpu.roll(packed, LANES - step, 1),
            pltpu.roll(packed, step, 1),
        )
        step *= 2
    stat[...] = packed

    pl.semaphore_wait(barrier, n_view - 1)

    def stat_copy(k):
        return pltpu.make_async_remote_copy(
            src_ref=stat, dst_ref=stat_in.at[k - 1], send_sem=stat_send, recv_sem=stat_recv,
            device_id={"view": lax.rem(me + k, n_view)},
        )

    def send_stat(k, carry):
        stat_copy(k).start()
        return carry

    lax.fori_loop(1, n_view, send_stat, 0, unroll=n_view <= 16)

    up_copy = pltpu.make_async_remote_copy(
        src_ref=lat.at[pl.ds(2, 2)], dst_ref=lat.at[pl.ds(rows + 2, 2)],
        send_sem=halo_send.at[0], recv_sem=halo_recv.at[0],
        device_id={"view": jnp.maximum(me - views, 0)},
    )
    down_copy = pltpu.make_async_remote_copy(
        src_ref=lat.at[pl.ds(rows, 2)], dst_ref=lat.at[pl.ds(0, 2)],
        send_sem=halo_send.at[1], recv_sem=halo_recv.at[1],
        device_id={"view": jnp.minimum(me + views, n_view - 1)},
    )

    @pl.when(has_up)
    def _():
        up_copy.start()

    @pl.when(has_down)
    def _():
        down_copy.start()

    for t in range(9):
        w2_copy(t).wait()
    piece = 32

    def fold_piece(k, carry):
        at = pl.ds(pl.multiple_of(k * piece, piece), piece)
        w = [w2[t, at].astype(F32) for t in range(9)]
        by_col = [w[s] + w[3 + s] + w[6 + s] for s in range(3)]
        fold[0, at] = (by_col[0] + by_col[1] + by_col[2]).astype(BF16)
        fold[1, at] = by_col[0].astype(BF16)
        fold[2, at] = by_col[2].astype(BF16)
        fold[3, at] = (w[0] + w[1] + w[2]).astype(BF16)
        fold[4, at] = (w[6] + w[7] + w[8]).astype(BF16)
        return carry

    lax.fori_loop(0, chans // piece, fold_piece, 0)

    pltpu.make_async_copy(stat_in, stat_in, stat_recv).wait()

    total = stat[...]
    total = total + jnp.sum(stat_in[...], axis=0)
    entries = float(own * (chans // GROUPS) * n_view)
    mean = total[:blocks] / entries
    var = total[blocks:] / entries - mean * mean
    inv = lax.rsqrt(var + EPSILON)

    def one_row(v):
        return jnp.concatenate([v[k : k + 1] for k in range(blocks)], axis=1)

    scale = one_row(inv) * gain_ref[...]
    offset = shift_ref[...] - one_row(mean) * scale

    col = lax.broadcasted_iota(jnp.int32, (cols, chans), 0)

    def left_of(x):
        return jnp.where(col == 0, 0.0, pltpu.roll(x, 1, 0))

    def right_of(x):
        return jnp.where(col == cols - 1, 0.0, pltpu.roll(x, cols - 1, 0))

    half_scale = scale * 0.5
    half_offset = offset * 0.5

    def activate(i, carry):
        h = lat[i].astype(F32) * half_scale + half_offset
        a = h + h * jnp.tanh(h)
        place = slab * rows + i - 2
        a = jnp.where(jnp.logical_and(place >= 0, place < H_LAT), a, 0.0)
        at = pl.ds(pl.multiple_of(i * cols, cols), cols)
        act[at, pl.ds(0, chans)] = left_of(a).astype(BF16)
        act[at, pl.ds(chans, chans)] = a.astype(BF16)
        act[at, pl.ds(2 * chans, chans)] = right_of(a).astype(BF16)
        return carry

    lax.fori_loop(2, rows + 2, activate, 0)
    for t in range(9):
        w1_copy(t).wait()
    deep = 3 * chans
    half = 256

    def taps(windows, n):
        lanes = pl.ds(n * half, half)
        terms = [
            dot_nt(
                jnp.concatenate([act[pl.ds(first + r * cols, size)] for first, size in windows], axis=0),
                w1[lanes, pl.ds(r * deep, deep)],
            )
            for r in range(3)
        ]
        return terms[0] + terms[1] + terms[2]

    for n in range(chans // half):
        acc[pl.ds(2 * cols, own - 2 * cols), pl.ds(n * half, half)] = taps([(2 * cols, own - 2 * cols)], n)

    @pl.when(has_up)
    def _():
        down_copy.wait_recv()

    @pl.when(has_down)
    def _():
        up_copy.wait_recv()

    lax.fori_loop(0, 2, activate, 0)
    lax.fori_loop(rows + 2, rows + 4, activate, 0)
    ends = [(0, 2 * cols), (own, 2 * cols)]
    for n in range(chans // half):
        term = taps(ends, n)
        for k, (first, size) in enumerate(ends):
            acc[pl.ds(first, size), pl.ds(n * half, half)] = term[k * size : (k + 1) * size]

    bias1 = b1_ref[...]

    def mixed_row(i):
        at = pl.ds(pl.multiple_of(i * cols, cols), cols)
        m = lat[i + 1].astype(F32) + acc[at] + bias1
        m = m.astype(BF16).astype(F32)
        place = slab * rows + i - 1
        return jnp.where(jnp.logical_and(place >= 0, place < H_LAT), m, 0.0)

    def spread(i, carry):
        m = mixed_row(i + 1)
        u = m - mixed_row(i)
        at = pl.ds(pl.multiple_of(i * cols, cols), cols)
        for ref, x in ((lhs_m, m), (lhs_u, u)):
            ref[0, at] = x.astype(BF16)
            ref[1, at] = (left_of(x) - x).astype(BF16)
            ref[2, at] = (right_of(x) - x).astype(BF16)
        return carry

    lax.fori_loop(0, rows + 1, spread, 0)

    width = 256

    for n in range(chans // width):
        lanes = pl.ds(n * width, width)
        head = pl.ds(0, own)
        base = dot_nt(lhs_m[0, head], fold[0, lanes]) + b2_ref[:, lanes]
        part[0] = base + dot_nt(lhs_m[1, head], fold[1, lanes])
        part[1] = base + dot_nt(lhs_m[2, head], fold[2, lanes])
        for p in range(2):
            at = pl.ds(p * cols, own)
            rise = dot_nt(lhs_u[0, at], fold[3 + p, lanes])
            for q in range(2):
                term = rise + dot_nt(lhs_u[1 + q, at], w2[6 * p + 2 * q, lanes])
                value = part[q] + term if p else part[q] - term
                for g in range(width // LANES):
                    wide[g, pl.ds(p * own * 2 + q, own, 2), :] = value[:, g * LANES : (g + 1) * LANES]
            for g in range(width // LANES):
                tile = wide[g, pl.ds(p * own * 2, own * 2), :].astype(BF16)
                out_ref[:, p, :, pl.ds(n * width + g * LANES, LANES)] = tile.reshape(rows, 2 * cols, LANES)

    pltpu.make_async_copy(stat_in, stat_in, stat_send).wait()

    @pl.when(has_up)
    def _():
        up_copy.wait_send()

    @pl.when(has_down)
    def _():
        down_copy.wait_send()


def per_device(n_view, latents, norm_gain, norm_shift, w_first, bias_first, w_second, bias_second):
    rows, cols, chans = latents.shape
    own = rows * cols
    flat = lambda w: jnp.transpose(w, (1, 2, 0, 3)).reshape(9, chans, chans)
    row = lambda v: v.reshape(1, chans)
    vmem = pl.BlockSpec(memory_space=pltpu.VMEM)
    hbm = pl.BlockSpec(memory_space=pl.ANY)
    out = pl.pallas_call(
        functools.partial(kernel, n_view, rows, cols, chans),
        out_shape=pltpu.VMEM((rows, 2, 2 * cols, chans), BF16),
        in_specs=[hbm, vmem, vmem, hbm, vmem, hbm, vmem],
        out_specs=vmem,
        scratch_shapes=[
            pltpu.VMEM((rows + 4, cols, chans), BF16),
            pltpu.VMEM((chans, 9 * chans), BF16),
            pltpu.VMEM((9, chans, chans), BF16),
            pltpu.VMEM((5, chans, chans), BF16),
            pltpu.VMEM(((rows + 4) * cols, 3 * chans), BF16),
            pltpu.VMEM(((rows + 2) * cols, chans), F32),
            pltpu.VMEM((3, own + cols, chans), BF16),
            pltpu.VMEM((3, own + cols, chans), BF16),
            pltpu.VMEM((2, own, 256), F32),
            pltpu.VMEM((2, own * 4, LANES), F32),
            pltpu.VMEM((2 * chans // LANES, LANES), F32),
            pltpu.VMEM((n_view - 1, 2 * chans // LANES, LANES), F32),
            pltpu.SemaphoreType.DMA,
            pltpu.SemaphoreType.DMA((9,)),
            pltpu.SemaphoreType.DMA((9,)),
            pltpu.SemaphoreType.DMA((2,)),
            pltpu.SemaphoreType.DMA((2,)),
            pltpu.SemaphoreType.DMA,
            pltpu.SemaphoreType.DMA,
        ],
        compiler_params=pltpu.CompilerParams(
            collective_id=0, has_side_effects=True, vmem_limit_bytes=60 * 1024 * 1024
        ),
    )(
        latents, row(norm_gain), row(norm_shift), flat(w_first), row(bias_first), flat(w_second),
        row(bias_second),
    )
    return out.reshape(2 * rows, 2 * cols, chans)


def solution(mesh):
    placed = (P(("scene", "view"), None, None), P(), P(), P(), P(), P(), P())
    return jax.shard_map(
        functools.partial(per_device, mesh.shape["view"]),
        mesh=mesh,
        in_specs=placed,
        out_specs=P(("scene", "view"), None, None),
        check_vma=False,
    )
```
